32 devices in a mesh: mem: 2 (over x), col: 16 (over z, y, core).
Axes of the slice: x: 2, y: 2, z: 4, core: 2. Of those that a mesh axis runs over, the one named last changes fastest.
Arguments:
- state_a: bfloat16 [64, 1048576], P('mem', 'col'), may hold values from -12 to 12
- state_b: bfloat16 [64, 1048576], P('mem', 'col'), may hold values from -12 to 12
- obs_index: int32 [2, 8192, 16], P(None, ('col', 'mem')), may hold values from 0 to 127
- observation_count: int32 [2, 8192], P(None, ('col', 'mem')), may hold values from 1 to 16, as said below
- obs_value: float32 [2, 8192, 16], P(None, ('col', 'mem')), may hold values from -32 to 32
- obs_weight: float32 [2, 8192, 16], P(None, ('col', 'mem')), may hold values from 0.02 to 0.2
Outputs:
- analysis_a: bfloat16 [64, 1048576], P(None, ('col', 'mem'))
- analysis_b: bfloat16 [64, 1048576], P(None, ('col', 'mem'))
- transform: float32 [64, 64], replicated
The draws below stay inside these ranges and needn't reach their ends.
Inputs may be any that keep to these rules, and one draw needn't show every extreme that they name: Slot s of block b of group g is an observation when s < observation_count[g, b]; for each group, every aligned run of 256 blocks holds a block with all 16 slots live.
All inputs are finite; a program needn't handle non-finite values.
Results may differ from the reference program's by a relative error of at most 0.005.
Values may be sent and summed in bfloat16 or wider, within the bound.
A program may use at most 64 MiB of HBM per device.

```python
import math
import jax
import jax.numpy as jnp
from jax import lax

K = 64
OBS_BLK = 16
ITERS = 24
NCOL = 1048576
PIECE = 32768
BPD = 256
NBLK = 8192


def group_parts(key, salt):
    key = jax.random.fold_in(key, salt)
    subkeys = jax.random.split(key, 8)
    patterns = jax.random.normal(subkeys[0], (K, 3), jnp.float32)
    amplitudes = jnp.exp(jax.random.uniform(subkeys[1], (3, 16), jnp.float32, jnp.log(0.2), jnp.log(1.6)))
    coefficients = jax.random.normal(subkeys[2], (3, NCOL), jnp.float32)
    scales = jnp.exp(jax.random.uniform(subkeys[3], (K,), jnp.float32, jnp.log(0.5), jnp.log(2.0)))
    member_noise = 0.5 * jax.random.normal(subkeys[4], (K, NCOL), jnp.float32)
    truth_noise = 0.5 * jax.random.normal(subkeys[5], (NCOL,), jnp.float32)
    offsets = jax.random.uniform(subkeys[6], (3,), jnp.float32, 1.0, 2.0)
    sign_flip = jnp.where(jax.random.uniform(subkeys[7], (3,), jnp.float32) < 0.5, -1.0, 1.0)
    driving = jnp.repeat(amplitudes, NCOL // 16, axis=1) * coefficients
    truth_coef = jnp.mean(patterns, axis=0) + offsets * sign_flip
    return (patterns, driving, scales, member_noise, truth_noise, truth_coef)


def member_field(key, salt):
    patterns, driving, scales, member_noise, truth_noise, truth_coef = group_parts(key, salt)
    member_values = scales[:, None] * member_noise + jnp.dot(patterns, driving, precision=lax.Precision.HIGHEST)
    return jnp.clip(member_values, -12.0, 12.0).astype(jnp.bfloat16)


def index_table(key):
    return jax.random.randint(jax.random.fold_in(key, 41), (2, NBLK, OBS_BLK), 0, 128).astype(jnp.int32)


def draw_state_a(key, part):
    return member_field(key, 11)


def draw_state_b(key, part):
    return member_field(key, 23)


def draw_obs_index(key, part):
    return index_table(key)


def draw_obs_value(key, part):
    observation_lookup = index_table(key)
    picked = []
    for group, salt in enumerate((11, 23)):
        patterns, driving, scales, member_noise, truth_noise, truth_coef = group_parts(key, salt)
        truth_field = jnp.dot(truth_coef, driving, precision=lax.Precision.HIGHEST) + truth_noise
        truth_field = jnp.clip(truth_field, -12.0, 12.0)
        picked.append(jnp.take_along_axis(truth_field.reshape(NBLK, 128), observation_lookup[group], axis=1))
    error_key = jax.random.fold_in(key, 53)
    errors = jnp.clip(jax.random.normal(error_key, (2, NBLK, OBS_BLK), jnp.float32), -4.0, 4.0)
    return jnp.stack(picked) + 5.0 * errors


def draw_observation_count(key, part):
    key = jax.random.fold_in(key, 37)
    first, second = jax.random.split(key)
    segs = NBLK // BPD
    counts = jax.random.randint(first, (2, segs, BPD), 1, OBS_BLK + 1)
    where_full = jax.random.randint(second, (2, segs, 1), 0, BPD)
    position = lax.broadcasted_iota(jnp.int32, (2, segs, BPD), 2)
    counts = jnp.where(position == where_full, OBS_BLK, counts)
    return counts.reshape(2, NBLK).astype(jnp.int32)


def level_of(stream_key, shape, cuts, low, top_value):
    def one(axis_at, blocks):
        heights = jax.random.uniform(jax.random.fold_in(jax.random.fold_in(stream_key, 6), axis_at), (blocks,), jnp.float32, low / len(cuts), top_value / len(cuts))
        return jnp.repeat(jnp.exp(heights), shape[axis_at] // blocks).reshape((-1,) + (1,) * (len(shape) - axis_at - 1))

    loudness = one(*cuts[0])
    for cut in cuts[1:]:
        loudness = loudness * one(*cut)
    return loudness


def setup_inputs(seed: int = 0) -> dict:
    splits = jax.random.split(jax.random.key(seed), 7)
    return {
        "state_a": draw_state_a(jax.random.fold_in(splits[6], 71), 0),
        "state_b": draw_state_b(jax.random.fold_in(splits[6], 71), 0),
        "obs_index": draw_obs_index(jax.random.fold_in(splits[6], 71), 0),
        "observation_count": draw_observation_count(jax.random.fold_in(splits[6], 71), 0),
        "obs_value": draw_obs_value(jax.random.fold_in(splits[6], 71), 0),
        "obs_weight": jnp.clip(jnp.exp(math.log(0.2) - 2.3025851 * jax.random.uniform(splits[5], (2, NBLK, OBS_BLK), jnp.float32) ** level_of(splits[5], (2, NBLK, OBS_BLK), ((1, 32),), -0.2, 0.2)), 0.02, 0.2),
    }


def inverse_root(amat):
    scale = jnp.sqrt(jnp.sum(amat * amat))
    eye = jnp.eye(amat.shape[0], dtype=jnp.float32)

    def forward_step(step, carry):
        yn, zn = carry
        tm = 1.5 * eye - 0.5 * jnp.dot(zn, yn, precision=lax.Precision.HIGHEST)
        return (jnp.dot(yn, tm, precision=lax.Precision.HIGHEST), jnp.dot(tm, zn, precision=lax.Precision.HIGHEST))
    yn, zn = lax.fori_loop(0, ITERS, forward_step, (amat / scale, eye))
    return (zn, scale)

def make_transform(gram_product, cross, misfit, total):
    members = gram_product.shape[0]
    scl = (members - 1.0) / total
    gs = scl * gram_product
    bs = scl * cross
    qval = scl * misfit
    tval = jnp.trace(gs)
    rho = (1.0 + qval / (members - 1.0)) / (1.0 + tval / (members - 1.0))
    amat = (members - 1.0) / rho * jnp.eye(members, dtype=jnp.float32) + gs
    zn, scale = inverse_root(amat)
    pmat = jnp.dot(zn, zn, precision=lax.Precision.HIGHEST) / scale
    wbar = jnp.dot(pmat, bs, precision=lax.Precision.HIGHEST)
    return jnp.sqrt(members - 1.0) * zn / jnp.sqrt(scale) + wbar[:, None]

def reference(state_a, state_b, obs_index, observation_count, obs_value, obs_weight):
    segs = NCOL // PIECE
    states = (state_a, state_b)

    def accumulate(carry, seg):
        gram_product, cross, misfit, total = carry
        for group in range(2):
            cols = lax.dynamic_slice_in_dim(states[group], seg * PIECE, PIECE, 1)
            idx = lax.dynamic_slice_in_dim(obs_index[group], seg * BPD, BPD, 0)
            cnt = lax.dynamic_slice_in_dim(observation_count[group], seg * BPD, BPD, 0)
            val = lax.dynamic_slice_in_dim(obs_value[group], seg * BPD, BPD, 0)
            wgt = lax.dynamic_slice_in_dim(obs_weight[group], seg * BPD, BPD, 0)
            live = (lax.broadcasted_iota(jnp.int32, (BPD, OBS_BLK), 1) < cnt[:, None]).astype(jnp.float32)
            blocks = cols.reshape(K, BPD, 128)
            hx = jnp.take_along_axis(blocks, jnp.broadcast_to(idx[None], (K, BPD, OBS_BLK)), axis=2).astype(jnp.float32)
            hmean = lax.optimization_barrier(jnp.mean(hx, axis=0))
            anomaly_rows = hx - hmean[None]
            innov = val - hmean
            wt = live * wgt
            scaled_anomaly = anomaly_rows * wt[None]
            gram_product = gram_product + jnp.einsum('nix,fix->nf', scaled_anomaly, anomaly_rows, precision=lax.Precision.HIGHEST)
            cross = cross + jnp.einsum('kbs,bs->k', scaled_anomaly, innov, precision=lax.Precision.HIGHEST)
            misfit = misfit + jnp.sum(wt * innov * innov)
            total = total + jnp.sum(live)
        return ((gram_product, cross, misfit, total), None)
    init = (jnp.zeros((K, K), jnp.float32), jnp.zeros((K,), jnp.float32), jnp.zeros((), jnp.float32), jnp.zeros((), jnp.float32))
    (gram_product, cross, misfit, total), _ = lax.scan(accumulate, init, jnp.arange(segs, dtype=jnp.int32))
    transform = make_transform(gram_product, cross, misfit, total)
    wb = transform.astype(jnp.bfloat16)
    column_total = lax.optimization_barrier(jnp.sum(wb.astype(jnp.float32), axis=0))
    ones = jnp.ones((K,), jnp.bfloat16)

    def analyse(state):

        def one_seg(seg):
            cols = lax.dynamic_slice_in_dim(state, seg * PIECE, PIECE, 1)
            xmean = jnp.dot(ones, cols, preferred_element_type=jnp.float32) / K
            mixed = jnp.dot(wb.T, cols, preferred_element_type=jnp.float32)
            return (mixed + xmean[None, :] * (1.0 - column_total)[:, None]).astype(jnp.bfloat16)
        pieces = lax.map(one_seg, jnp.arange(segs, dtype=jnp.int32))
        return jnp.transpose(pieces, (1, 0, 2)).reshape(K, NCOL)
    return (analyse(state_a), analyse(state_b), transform)
```

```python
import functools

import jax
import jax.numpy as jnp
from jax import lax
from jax.experimental import pallas as pl
from jax.experimental.pallas import tpu as pltpu
from jax.sharding import PartitionSpec as P

ITERS = 24
LANES = 128
HIGH = lax.Precision.HIGHEST
MESH = pl.DeviceIdType.MESH
ROWS = 128
CHUNK = 2048
FIRST_PART = 0.34
HX_CUTS = 4


def bits(n):
    return [1 << i for i in range(n.bit_length() - 1)]


def transform_of(gram, members):
    members = members
    g = gram[:members, :members]
    cross = gram[members : members + 1, :members]
    misfit = gram[members : members + 1, members : members + 1]
    total = gram[members + 1 : members + 2, members + 1 : members + 2]
    rows = lax.broadcasted_iota(jnp.int32, (members, members), 0)
    cols = lax.broadcasted_iota(jnp.int32, (members, members), 1)
    eye = (rows == cols).astype(jnp.float32)

    def whole(x):
        return jnp.sum(jnp.sum(x, axis=1, keepdims=True), axis=0, keepdims=True)

    def parts(x):
        hi = x.astype(jnp.bfloat16)
        rest = x - hi.astype(jnp.float32)
        mid = rest.astype(jnp.bfloat16)
        low = (rest - mid.astype(jnp.float32)).astype(jnp.bfloat16)
        return hi, mid, low

    def dot(a, b):
        total = None
        for i in range(3):
            left = jnp.concatenate(a[: 3 - i], axis=0) if i < 2 else a[0]
            out = jnp.dot(left, b[i], preferred_element_type=jnp.float32)
            for j in reversed(range(3 - i)):
                block = out[j * members : (j + 1) * members]
                total = block if total is None else total + block
        return total

    dof = members - 1.0
    scl = dof / total
    gs = scl * g
    bs = scl * cross
    rho = (1.0 + scl * misfit / dof) / (1.0 + whole(gs * eye) / dof)
    amat = dof / rho * eye + gs
    scale = jnp.sqrt(whole(amat * amat))

    def step(_, carry):
        yn, zn = carry
        yp, zp = parts(yn), parts(zn)
        tp = parts(1.5 * eye - 0.5 * dot(zp, yp))
        return dot(yp, tp), dot(tp, zp)

    _, zn = lax.fori_loop(0, ITERS, step, (amat / scale, eye))
    zp = parts(zn)
    wbar = jnp.sum(dot(zp, zp) / scale * bs, axis=1, keepdims=True)
    return jnp.sqrt(dof) * zn / jnp.sqrt(scale) + wbar


def exchange_kernel(
    nmem, ncol, sa, sb, idx, val, wgt, cnt, ra, rb, tr,
    st, idx_in, hx, cur, got, load_sem, own_sem, idx_s, idx_r, hx_s, hx_r, st_s, st_r, red_s, red_r,
):
    me = lax.axis_index("mem")
    col = lax.axis_index("col")
    mk = sa.shape[0]
    members = mk * nmem
    piece = sa.shape[1] // nmem
    width = idx.shape[1]
    half = width // 2
    states, received = (sa, sb), (ra, rb)
    chunk = min(CHUNK, piece)
    cuts = piece // chunk
    peers = [lax.rem(me + d, nmem) for d in range(1, nmem)]
    across = [{"mem": me ^ b} for b in bits(nmem)] + [{"col": col ^ b} for b in bits(ncol)]
    col_peers = [col ^ b for b in bits(ncol)]

    def cols_of(owner, start, size):
        return pl.ds(pl.multiple_of(owner * piece + start, LANES), size)

    my_rows = pl.ds(pl.multiple_of(me * mk, mk), mk)

    loads = []
    for d in range(nmem):
        owner = peers[d - 1] if d else me
        for g in range(2):
            loads.append(
                pltpu.make_async_copy(
                    states[g].at[:, cols_of(owner, 0, piece)],
                    st.at[g, :, cols_of(owner, 0, piece)],
                    load_sem.at[d, g],
                )
            )
            loads[-1].start()

    barrier = pltpu.get_barrier_semaphore()
    for p in peers:
        pl.semaphore_signal(barrier, inc=1, device_id={"mem": p}, device_id_type=MESH)
    for c in col_peers:
        pl.semaphore_signal(barrier, inc=1, device_id={"col": c}, device_id_type=MESH)
    pl.semaphore_wait(barrier, len(peers) + len(col_peers))

    index_copies = []
    for d, p in enumerate(peers):
        index_copies.append(
            pltpu.make_async_remote_copy(
                idx, idx_in.at[d], idx_s.at[d], idx_r.at[d], device_id={"mem": p}, device_id_type=MESH
            )
        )
        index_copies[-1].start()

    moves = []
    for q in range(cuts):
        for g in range(2):
            for d, p in enumerate(peers):
                n = len(moves)
                moves.append(
                    pltpu.make_async_remote_copy(
                        states[g].at[:, cols_of(p, q * chunk, chunk)],
                        received[g].at[my_rows, pl.ds(q * chunk, chunk)],
                        st_s.at[n],
                        st_r.at[n],
                        device_id={"mem": p},
                        device_id_type=MESH,
                    )
                )
    first = int(len(moves) * FIRST_PART)
    for m in moves[:first]:
        m.start()

    def gather(index, owner, start, size, put):
        lane = lax.broadcasted_iota(jnp.int32, (mk, LANES), 1) // 16

        def row(r, _):
            at = pl.multiple_of(start + r * LANES, LANES)
            g = start // half
            base = (at - g * half) * 8
            s = st[g, :, cols_of(owner, base, 8 * LANES)].astype(jnp.float32)
            ir = jnp.broadcast_to(index[:, pl.ds(at, LANES)], (mk, LANES))
            out = jnp.zeros((mk, LANES), jnp.float32)
            for j in range(8):
                picked = jnp.take_along_axis(s[:, j * LANES : (j + 1) * LANES], ir, axis=1)
                out = jnp.where(lane == j, picked, out)
            put(pl.ds(at, LANES), out.astype(jnp.bfloat16))
            return 0

        lax.fori_loop(0, size // LANES, row, 0)

    step = width // HX_CUTS
    hx_copies = []
    for d, p in enumerate(peers):
        for g in range(2):
            loads[2 * (d + 1) + g].wait()
        index_copies[nmem - 2 - d].wait()
        for h in range(HX_CUTS):

            def put(where, value):
                hx[nmem + d, :, where] = value

            gather(idx_in.at[nmem - 2 - d], p, h * step, step, put)
            hx_copies.append(
                pltpu.make_async_remote_copy(
                    hx.at[nmem + d, :, pl.ds(h * step, step)],
                    hx.at[me, :, pl.ds(h * step, step)],
                    hx_s.at[d, h],
                    hx_r.at[d, h],
                    device_id={"mem": p},
                    device_id_type=MESH,
                )
            )
            if len(hx_copies) > 1:
                hx_copies[-2].start()
    for g in range(2):
        loads[g].wait()
    keep = []
    for g in range(2):
        keep.append(
            pltpu.make_async_copy(
                st.at[g, :, cols_of(me, 0, piece)], received[g].at[my_rows, :], own_sem.at[g]
            )
        )
        keep[-1].start()

    def put_own(where, value):
        hx[me, :, where] = value

    gather(idx, me, 0, step, put_own)
    hx_copies[-1].start()
    for h in range(1, HX_CUTS):
        gather(idx, me, h * step, step, put_own)
    for c in hx_copies:
        c.wait()

    span = min(1024, half)

    def accumulate(i, acc):
        where = pl.ds(pl.multiple_of(i * span, LANES), span)
        x = jnp.concatenate([hx[m, :, where].astype(jnp.float32) for m in range(nmem)], axis=0)
        hmean = jnp.sum(x, axis=0, keepdims=True) / members
        rest = jnp.zeros((ROWS - members - 1, span), jnp.float32)
        aug = jnp.concatenate([x - hmean, val[:, where] - hmean, rest], axis=0)
        return acc + lax.dot_general(
            aug * wgt[:, where], aug, (((1,), (1,)), ((), ())), precision=HIGH,
            preferred_element_type=jnp.float32,
        )

    gram = lax.fori_loop(0, width // span, accumulate, jnp.zeros((ROWS, ROWS), jnp.float32))
    live = cnt[...].astype(jnp.float32)
    live = jnp.sum(jnp.sum(live, axis=1, keepdims=True), axis=0, keepdims=True)
    rows = lax.broadcasted_iota(jnp.int32, (ROWS, ROWS), 0)
    cols = lax.broadcasted_iota(jnp.int32, (ROWS, ROWS), 1)
    gram = jnp.where((rows == members + 1) & (cols == members + 1), live, gram)
    cur[0] = gram
    started = len(moves) if not bits(nmem) else first
    for s, peer in enumerate(across):
        copy = pltpu.make_async_remote_copy(
            cur.at[s], got.at[s], red_s.at[s], red_r.at[s], device_id=peer, device_id_type=MESH
        )
        copy.start()
        if s + 1 == len(bits(nmem)):
            for m in moves[started:]:
                m.start()
        copy.wait()
        cur[s + 1] = cur[s] + got[s]
    tr[...] = transform_of(cur[len(across)], members)
    for c in keep:
        c.wait()
    for m in moves:
        m.wait()


def exchange(state_a, state_b, idx, val, wgt, cnt):
    nmem, ncol = lax.axis_size("mem"), lax.axis_size("col")
    mk, held = state_a.shape
    piece = held // nmem
    width = idx.shape[1]
    members = mk * nmem
    steps = len(bits(nmem)) + len(bits(ncol))
    moves = 2 * (nmem - 1) * (piece // min(CHUNK, piece))
    dma = pltpu.SemaphoreType.DMA
    hbm = pl.BlockSpec(memory_space=pl.ANY)
    vmem = pl.BlockSpec(memory_space=pltpu.VMEM)
    return pl.pallas_call(
        functools.partial(exchange_kernel, nmem, ncol),
        out_shape=(
            jax.ShapeDtypeStruct((members, piece), jnp.bfloat16),
            jax.ShapeDtypeStruct((members, piece), jnp.bfloat16),
            jax.ShapeDtypeStruct((members, members), jnp.float32),
        ),
        in_specs=[hbm, hbm, vmem, vmem, vmem, vmem],
        out_specs=(hbm, hbm, vmem),
        scratch_shapes=[
            pltpu.VMEM((2, mk, held), jnp.bfloat16),
            pltpu.VMEM((nmem - 1, 1, width), jnp.int32),
            pltpu.VMEM((2 * nmem - 1, mk, width), jnp.bfloat16),
            pltpu.VMEM((steps + 1, ROWS, LANES), jnp.float32),
            pltpu.VMEM((steps, ROWS, LANES), jnp.float32),
            dma((nmem, 2)),
            dma((2,)),
            dma((nmem - 1,)),
            dma((nmem - 1,)),
            dma((nmem - 1, HX_CUTS)),
            dma((nmem - 1, HX_CUTS)),
            dma((moves,)),
            dma((moves,)),
            dma((steps,)),
            dma((steps,)),
        ],
        compiler_params=pltpu.CompilerParams(
            collective_id=0, has_side_effects=True, vmem_limit_bytes=62 * 2**20
        ),
        name="exchange",
    )(state_a, state_b, idx, val, wgt, cnt)


def apply_kernel(tr, xa, xb, oa, ob, lhs, coef):
    members = tr.shape[0]

    @pl.when(pl.program_id(0) == 0)
    def _():
        wt = tr[...].T.astype(jnp.bfloat16)
        lhs[:members, :] = wt
        lhs[members:, :] = jnp.full((16, members), 1.0 / members, jnp.bfloat16)
        coef[...] = 1.0 - jnp.sum(wt.astype(jnp.float32), axis=1, keepdims=True)

    for x, o in ((xa, oa), (xb, ob)):
        mixed = jnp.dot(lhs[...], x[...], preferred_element_type=jnp.float32)
        xmean = mixed[members : members + 1]
        o[...] = (mixed[:members] + coef[...] * xmean).astype(o.dtype)


def apply(tr, xa, xb):
    members, piece = xa.shape
    block = min(4096, piece)
    wide = pl.BlockSpec((members, block), lambda i: (0, i))
    return pl.pallas_call(
        apply_kernel,
        grid=(piece // block,),
        out_shape=(jax.ShapeDtypeStruct(xa.shape, xa.dtype),) * 2,
        in_specs=[pl.BlockSpec((members, members), lambda i: (0, 0)), wide, wide],
        out_specs=(wide, wide),
        scratch_shapes=[
            pltpu.VMEM((members + 16, members), jnp.bfloat16),
            pltpu.VMEM((members, 1), jnp.float32),
        ],
        compiler_params=pltpu.CompilerParams(dimension_semantics=("arbitrary",)),
        name="apply",
    )(tr, xa, xb)


def shards(state_a, state_b, obs_index, observation_count, obs_value, obs_weight):
    nblk, slots = obs_index.shape[1:]
    width = 2 * nblk * slots
    live = lax.broadcasted_iota(jnp.int32, obs_weight.shape, 2) < observation_count[:, :, None]
    weights = jnp.where(live, obs_weight, 0.0).reshape(1, width)
    ra, rb, transform = exchange(
        state_a, state_b, obs_index.reshape(1, width), obs_value.reshape(1, width), weights,
        observation_count,
    )
    out_a, out_b = apply(transform, ra, rb)
    return (out_a, out_b, transform)


def solution(mesh):
    return jax.shard_map(
        shards,
        mesh=mesh,
        in_specs=(
            P("mem", "col"),
            P("mem", "col"),
            P(None, ("col", "mem"), None),
            P(None, ("col", "mem")),
            P(None, ("col", "mem"), None),
            P(None, ("col", "mem"), None),
        ),
        out_specs=(P(None, ("col", "mem")), P(None, ("col", "mem")), P()),
        check_vma=False,
    )
```
